256 devices in a mesh: row: 8 (over y, core), col: 32 (over x, z).
Axes of the slice: x: 4, y: 4, z: 8, core: 2. Of those that a mesh axis runs over, the one named last changes fastest.
Arguments:
- phases: int32 [8, 32, 8, 24, 576], P('row', 'col'), may hold values from 0 to 2
- grain: float32 [8, 32, 8, 24, 576], P('row', 'col'), may hold values from 0.5 to 2
- phase_cond: float32 [3], replicated, may hold values from 0.3 to 3
- micro_counts: int32 [8, 32, 8], P('row', 'col'), may hold values from 6 to 12, as said below
- current: float32 [8, 32, 8], P('row', 'col'), may hold values from -5 to 5
- load: float32 [8, 32, 8], P('row', 'col'), may hold values from -16 to 16
Outputs:
- states: float32 [8, 32, 8, 3, 24, 576], P('row', 'col')
- tangent: float32 [8, 32, 8, 3, 3], P('row', 'col')
- increment: float32 [8, 32, 8], P('row', 'col')
- residual: float32 [8, 32, 8], P('row', 'col')
The draws below stay inside these ranges and needn't reach their ends.
Inputs may be any that keep to these rules, and one draw needn't show every extreme that they name: `micro_counts`: every draw has an element with 12 inner iterations and one with 6.
All inputs are finite; a program needn't handle non-finite values.
Results may differ from the reference program's by a relative error of at most 0.0003.
Values sent between devices are 32-bit elements; how exact they have to be, the bound alone decides.
A program may use at most 64 MiB of HBM per device.

```python
import math
import jax
import jax.numpy as jnp
from jax import lax

VOX = 24
YZ = 576
PHASES = 3
EZ = 8
MICRO_MAX = 12
MICRO_MIN = 6
MACRO_ITERS = 8
NEX = 8
NEY = 32


def draw_micro_counts(key, part):
    first_key, second_key = jax.random.split(jax.random.fold_in(key, 11))
    base = jax.random.randint(first_key, (NEX, NEY, 1), MICRO_MIN, MICRO_MAX + 1)
    jitter = jax.random.randint(second_key, (NEX, NEY, EZ), -1, 2)
    counts = jnp.clip(base + jitter, MICRO_MIN, MICRO_MAX)
    counts = counts.at[0, 0, 0].set(MICRO_MAX).at[0, 0, 1].set(MICRO_MIN)
    return counts.astype(jnp.int32)


def draw_load(key, part):
    along_x = jnp.arange(NEX, dtype=jnp.float32)[:, None, None] / (NEX - 1)
    along_y = jnp.arange(NEY, dtype=jnp.float32)[None, :, None] / (NEY - 1)
    scale = (1.0 + along_x) * (1.0 + along_y)
    sub_key = jax.random.fold_in(key, 23)
    values = jnp.clip(jax.random.normal(sub_key, (NEX, NEY, EZ), jnp.float32), -4.0, 4.0)
    return (scale * values).astype(jnp.float32)


def plant(entries, own_key, least, high):
    spot = [jax.random.randint(jax.random.fold_in(own_key, axis), (), 0, length) for axis, length in enumerate(entries.shape)]
    longest = entries.shape.index(max(entries.shape))
    next_to = spot[:longest] + [(spot[longest] + 1) % entries.shape[longest]] + spot[longest + 1:]
    return entries.at[tuple(spot)].set(least).at[tuple(next_to)].set(high)


def block_levels(stream_key, extent, shards, least, top_value):
    def one(position, shards_of):
        heights = jax.random.uniform(jax.random.fold_in(jax.random.fold_in(stream_key, 6), position), (shards_of,), jnp.float32, least / len(shards), top_value / len(shards))
        return jnp.repeat(jnp.exp(heights), extent[position] // shards_of).reshape((-1,) + (1,) * (len(extent) - position - 1))

    loudness = one(*shards[0])
    for cut in shards[1:]:
        loudness = loudness * one(*cut)
    return loudness


def noise(rng, shape, deviation, most, cuts=(), kind=jnp.bfloat16):
    gain = block_levels(rng, shape, cuts, -0.22, 0.18) if cuts else 1.0
    entries = jax.random.normal(rng, shape, jnp.float32) * deviation * gain
    return jnp.minimum(jnp.maximum(entries, -most), most).astype(kind)


def setup_inputs(seed: int = 0) -> dict:
    seeds = jax.random.split(jax.random.key(seed), 7)
    phases = plant(jax.random.randint(seeds[0], (NEX, NEY, EZ, VOX, YZ), 0, PHASES), jax.random.fold_in(seeds[0], 1), 0, PHASES - 1).astype(jnp.int32)
    grain = jnp.clip(jnp.exp(math.log(2.0) - 1.3862944 * jax.random.uniform(seeds[1], (NEX, NEY, EZ, VOX, YZ), jnp.float32) ** block_levels(seeds[1], (NEX, NEY, EZ, VOX, YZ), ((0, 8), (1, 32)), -0.2, 0.2)), 0.5, 2.0)
    phase_cond = jnp.clip(jnp.exp(jax.random.uniform(seeds[2], (PHASES,), jnp.float32, math.log(0.3), math.log(3.0))), 0.3, 3.0)
    micro_counts = draw_micro_counts(jax.random.fold_in(seeds[6], 71), 0)
    current = noise(seeds[4], (NEX, NEY, EZ), 1.0, 5.0, ((0, 8), (1, 32)), jnp.float32)
    load = draw_load(jax.random.fold_in(seeds[6], 71), 0)
    return {"phases": phases, "grain": grain, "phase_cond": phase_cond, "micro_counts": micro_counts, "current": current, "load": load}


def forward(field, axis_id):
    z_index = jnp.arange(YZ) % VOX
    if axis_id == 0:
        return jnp.roll(field, -1, axis=-2)
    if axis_id == 1:
        return jnp.roll(field, -VOX, axis=-1)
    return jnp.where(z_index == VOX - 1, jnp.roll(field, VOX - 1, axis=-1), jnp.roll(field, -1, axis=-1))


def behind(field, axis_id):
    z_index = jnp.arange(YZ) % VOX
    if axis_id == 0:
        return jnp.roll(field, 1, axis=-2)
    if axis_id == 1:
        return jnp.roll(field, VOX, axis=-1)
    return jnp.where(z_index == 0, jnp.roll(field, 1 - VOX, axis=-1), jnp.roll(field, 1, axis=-1))


def solve_rve(conduct, count):
    faces = [(conduct + forward(conduct, axis_id)) * 0.5 for axis_id in range(3)]
    back_faces = [behind(faces[axis_id], axis_id) for axis_id in range(3)]
    rhs = jnp.stack([faces[axis_id] - back_faces[axis_id] for axis_id in range(3)])

    def operate(field):
        total = jnp.zeros_like(field)
        for axis_id in range(3):
            total = total + faces[axis_id] * (field - forward(field, axis_id))
            total = total + back_faces[axis_id] * (field - behind(field, axis_id))
        return total

    def sweep(index, carry):
        fluct, remain, direction, norm_now = carry
        image = operate(direction)
        step_size = norm_now / jnp.sum(direction * image, axis=(1, 2))
        fluct = fluct + step_size[:, None, None] * direction
        remain = remain - step_size[:, None, None] * image
        norm_next = jnp.sum(remain * remain, axis=(1, 2))
        direction = remain + (norm_next / norm_now)[:, None, None] * direction
        return fluct, remain, direction, norm_next

    start = (jnp.zeros_like(rhs), rhs, rhs, jnp.sum(rhs * rhs, axis=(1, 2)))
    fluct = lax.fori_loop(0, count, sweep, start)[0]
    identity = jnp.eye(3, dtype=conduct.dtype)
    rows_out = []
    for axis_id in range(3):
        flux = faces[axis_id][None] * (identity[axis_id][:, None, None] + forward(fluct, axis_id) - fluct)
        rows_out.append(jnp.mean(flux, axis=(1, 2)))
    return fluct, jnp.stack(rows_out)


def neighbour(padded, axis_id, offset):
    lead = padded.ndim - 3
    index = [slice(None)] * lead + [slice(1, -1)] * 3
    length = padded.shape[lead + axis_id]
    index[lead + axis_id] = slice(1 + offset, length - 1 + offset)
    return padded[tuple(index)]


def coarse_apply(k_padded, v_padded):
    centre = neighbour(v_padded, 0, 0)
    total = jnp.zeros_like(centre)
    for axis_id in range(3):
        k_centre = neighbour(k_padded[axis_id], 0, 0)
        for offset in (1, -1):
            cond_face = 0.5 * (k_centre + neighbour(k_padded[axis_id], axis_id, offset))
            total = total + cond_face * (centre - neighbour(v_padded, axis_id, offset))
    return total


def reference(phases, grain, phase_cond, micro_counts, current, load):
    conduct = jnp.zeros(grain.shape, grain.dtype)
    for phase_id in range(PHASES):
        conduct = conduct + jnp.where(phases == phase_id, phase_cond[phase_id], 0.0)
    conduct = conduct * grain
    flat = conduct.reshape(-1, VOX, YZ)
    counts = micro_counts.reshape(-1).astype(jnp.int32)
    fluct, tangent = lax.map(lambda pair: solve_rve(pair[0], pair[1]), (flat, counts))
    states = fluct.reshape(NEX, NEY, EZ, 3, VOX, YZ)
    tangent = tangent.reshape(NEX, NEY, EZ, 3, 3)
    diag = jnp.stack([tangent[..., axis_id, axis_id] for axis_id in range(3)])
    k_padded = jnp.pad(diag, ((0, 0), (1, 1), (1, 1), (1, 1)))
    residual = load - coarse_apply(k_padded, jnp.pad(current, 1))
    increment = jnp.zeros_like(residual)
    direction = residual
    norm_now = jnp.sum(residual * residual)
    for iteration in range(MACRO_ITERS):
        image = coarse_apply(k_padded, jnp.pad(direction, 1))
        step_size = norm_now / jnp.sum(direction * image)
        increment = increment + step_size * direction
        residual = residual - step_size * image
        norm_next = jnp.sum(residual * residual)
        direction = residual + (norm_next / norm_now) * direction
        norm_now = norm_next
    return states, tangent, increment, residual
```

```python
import functools

import jax
import jax.numpy as jnp
from jax import lax
from jax.experimental import pallas as pl
from jax.experimental.pallas import tpu as pltpu
from jax.sharding import PartitionSpec as P

VOX = 24
YZ = 576
PHASES = 3
MACRO_ITERS = 8
MICRO_MAX = 12

XC, YC, ZC = 3, 12, 3
ELEMENTS = 8
HALF = YZ // 2
SPANS = ((0, 128), (128, 128), (256, 32))


def swap_half(value):
    lane = lax.broadcasted_iota(jnp.int32, value.shape, 1)
    return jnp.where((lane & 8) == 0, pltpu.roll(value, 120, 1), pltpu.roll(value, 8, 1))


def next_x(value):
    return pltpu.roll(value, 112, 1)


def prev_x(value):
    return pltpu.roll(value, 16, 1)


def next_z(value):
    return pltpu.roll(value, 7, 0)


def prev_z(value):
    return pltpu.roll(value, 1, 0)


def total_of(value):
    for shift in (1, 2, 4):
        value = value + pltpu.roll(value, shift, 0)
    for shift in (8, 16, 32, 64):
        value = value + pltpu.roll(value, shift, 1)
    return value


SPOTS = [(xc, zc) for xc in range(XC) for zc in range(ZC)]


def plane(ref, yc, lead=()):
    return {(xc, zc): ref[(*lead, xc, yc, zc)] for xc, zc in SPOTS}


def ahead_x(values, xc, zc):
    return values[xc + 1, zc] if xc < XC - 1 else next_x(values[0, zc])


def back_x(values, xc, zc):
    return values[xc - 1, zc] if xc > 0 else prev_x(values[XC - 1, zc])


def ahead_z(values, xc, zc):
    return values[xc, zc + 1] if zc < ZC - 1 else next_z(values[xc, 0])


def back_z(values, xc, zc):
    return values[xc, zc - 1] if zc > 0 else prev_z(values[xc, ZC - 1])


def swapped(values):
    return {spot: swap_half(value) for spot, value in values.items()}


class Sum:
    def __init__(self, ways=4):
        self.parts = [None] * ways
        self.at = 0

    def add(self, value):
        slot = self.at % len(self.parts)
        self.at += 1
        self.parts[slot] = value if self.parts[slot] is None else self.parts[slot] + value

    def get(self):
        parts = [part for part in self.parts if part is not None]
        while len(parts) > 1:
            parts = [sum(parts[i : i + 2][1:], parts[i]) for i in range(0, len(parts), 2)]
        return parts[0]


def far_first(nrow, ncol):
    ny, nx = nrow // 2, 4
    nz = ncol // nx
    offsets = [
        (y, core, x, z) for y in range(ny) for core in range(2) for x in range(nx) for z in range(nz)
    ]

    def hops(offset):
        y, core, x, z = offset
        return min(y, ny - y) + min(x, nx - x) + min(z, nz - z) + 0.5 * core

    return sorted(offsets[1:], key=hops, reverse=True)


def peer_of(row, col, offset, nrow, ncol):
    ny, nx = nrow // 2, 4
    nz = ncol // nx
    y, core, x, z = offset
    return {
        "row": lax.rem(row // 2 + y, ny) * 2 + lax.rem(row + core, 2),
        "col": lax.rem(col // nz + x, nx) * nz + lax.rem(lax.rem(col, nz) + z, nz),
    }


def fused_kernel(
    nrow, ncol,
    phases_ref, grain_ref, pc_ref, counts_ref, current_ref, load_ref, states_ref, tangent_ref, table_ref,
    rows, turned, cond, faces, rhs, fluct, remain, direction, image, scal, mine, got, own_sem, send_sem, recv_sem,
):
    n = nrow * ncol
    row, col = lax.axis_index("row"), lax.axis_index("col")
    offsets = far_first(nrow, ncol)
    barrier = pltpu.get_barrier_semaphore()
    for offset in offsets:
        pl.semaphore_signal(
            barrier, inc=1, device_id=peer_of(row, col, offset, nrow, ncol), device_id_type=pl.DeviceIdType.MESH
        )

    pc = [pc_ref[k] for k in range(PHASES)]
    for e in range(ELEMENTS):
        phase = phases_ref[0, 0, e]
        value = jnp.where(phase == 0, pc[0], jnp.where(phase == 1, pc[1], pc[2])) * grain_ref[0, 0, e]
        for yh in range(2):
            base = (yh * ELEMENTS + e) * VOX
            for t, (start, size) in enumerate(SPANS):
                rows[t, base : base + VOX, 0:size] = value[:, yh * HALF + start : yh * HALF + start + size]
    for xc in range(XC):
        for t, (start, size) in enumerate(SPANS):
            parts = []
            for xs in range(8):
                for yh in range(2):
                    parts.append(rows.at[t][pl.ds(yh * ELEMENTS * VOX + 3 * xs + xc, 8, stride=VOX), :])
            block = jnp.concatenate(parts, axis=0).T
            turned[xc * HALF + start : xc * HALF + start + size, :] = block[0:size]
    for xc in range(XC):
        for yc in range(YC):
            for zc in range(ZC):
                cond[xc, yc, zc] = turned[pl.ds(xc * HALF + yc * VOX + zc, 8, stride=3), :]

    face_sums = [Sum(), Sum(), Sum()]
    here = plane(cond, 0)
    for yc in range(YC):
        ahead = plane(cond, yc + 1) if yc < YC - 1 else swapped(plane(cond, 0))
        for xc, zc in SPOTS:
            own = here[xc, zc]
            for d, other in enumerate((ahead_x(here, xc, zc), ahead[xc, zc], ahead_z(here, xc, zc))):
                face = (own + other) * 0.5
                faces[d, xc, yc, zc] = face
                face_sums[d].add(face)
        here = ahead
    norms = [Sum(), Sum(), Sum()]
    before = swapped(plane(faces, YC - 1, (1,)))
    for yc in range(YC):
        fx, fy, fz = (plane(faces, yc, (d,)) for d in range(3))
        for xc, zc in SPOTS:
            backs = (back_x(fx, xc, zc), before[xc, zc], back_z(fz, xc, zc))
            for d, own in enumerate((fx[xc, zc], fy[xc, zc], fz[xc, zc])):
                value = own - backs[d]
                rhs[d, xc, yc, zc] = value
                remain[d, xc, yc, zc] = value
                norms[d].add(value * value)
        before = fy

    lane = lax.broadcasted_iota(jnp.int32, (8, 128), 1)
    counts = jnp.zeros((8, 128), jnp.int32)
    coarse = [jnp.zeros((8, 128), jnp.float32)] * 2
    for e in range(ELEMENTS):
        here_e = (lane & 7) == e
        counts = jnp.where(here_e, counts_ref[0, 0, e], counts)
        coarse = [jnp.where(here_e, ref[0, 0, e], value) for ref, value in zip((current_ref, load_ref), coarse)]

    def sweep(c, alpha, beta, first):
        curv = Sum()

        def fresh(yc):
            out = {}
            for xc, zc in SPOTS:
                at = (c, xc, yc, zc)
                if first:
                    value = remain[at]
                    fluct[at] = jnp.zeros((8, 128), jnp.float32)
                else:
                    old = direction[at]
                    fluct[at] = fluct[at] + alpha * old
                    value = remain[at] + beta * old
                direction[at] = value
                out[xc, zc] = value
            return out

        last = fresh(YC - 1)
        here = fresh(0)
        flow_back = {
            s: swap_half(faces[1, s[0], YC - 1, s[1]] * (last[s] - swap_half(here[s]))) for s in SPOTS
        }
        for yc in range(YC):
            if yc < YC - 2:
                ahead = fresh(yc + 1)
            elif yc == YC - 2:
                ahead = plane(direction, YC - 1, (c,))
            else:
                ahead = swapped(plane(direction, 0, (c,)))
            gx, gy, gz = {}, {}, {}
            for xc, zc in SPOTS:
                own = here[xc, zc]
                gx[xc, zc] = faces[0, xc, yc, zc] * (own - ahead_x(here, xc, zc))
                gy[xc, zc] = faces[1, xc, yc, zc] * (own - ahead[xc, zc])
                gz[xc, zc] = faces[2, xc, yc, zc] * (own - ahead_z(here, xc, zc))
            for xc, zc in SPOTS:
                value = (
                    (gx[xc, zc] - back_x(gx, xc, zc))
                    + (gy[xc, zc] - flow_back[xc, zc])
                    + (gz[xc, zc] - back_z(gz, xc, zc))
                )
                image[c, xc, yc, zc] = value
                curv.add(here[xc, zc] * value)
            flow_back = gy
            here = ahead
        return total_of(curv.get())

    def reduce_residual(c, alpha):
        norm = Sum()
        for yc in range(YC):
            for xc, zc in SPOTS:
                at = (c, xc, yc, zc)
                value = remain[at] - alpha * image[at]
                remain[at] = value
                norm.add(value * value)
        return total_of(norm.get())

    for c in range(3):
        norm = total_of(norms[c].get())
        curv = sweep(c, None, None, True)
        scal[0, c] = norm
        alpha = norm / curv
        scal[1, c] = alpha
        scal[2, c] = alpha * norm

    def iterate(index, carry):
        for c in range(3):
            alpha = scal[1, c]
            norm = scal[0, c]
            norm_next = reduce_residual(c, alpha)
            active = index < counts
            curv = sweep(c, alpha, jnp.where(active, norm_next / norm, 0.0), False)
            scal[0, c] = norm_next
            alpha = jnp.where(active, norm_next / curv, 0.0)
            scal[1, c] = alpha
            scal[2, c] = scal[2, c] + alpha * norm_next
        return carry

    lax.fori_loop(1, MICRO_MAX, iterate, 0)

    scale = 1.0 / (VOX * YZ)
    face_totals = [total_of(part.get()) for part in face_sums]
    fields = [(face_totals[d] - scal[2, d]) * scale for d in range(3)] + coarse
    slot = ((lane >> 3) - col) & 15
    packed = fields[4]
    for f in range(4):
        packed = jnp.where(slot == f, fields[f], packed)
    mine[...] = packed[0:1]

    me = col * nrow + row
    pl.semaphore_wait(barrier, n - 1)
    got[pl.ds(me, 1)] = packed[0:1]
    for offset in offsets:
        pltpu.make_async_remote_copy(
            src_ref=mine,
            dst_ref=got.at[pl.ds(me, 1)],
            send_sem=send_sem,
            recv_sem=recv_sem,
            device_id=peer_of(row, col, offset, nrow, ncol),
            device_id_type=pl.DeviceIdType.MESH,
        ).start()

    entries = {}
    for c in range(3):
        alpha = scal[1, c]
        sums = [Sum(2), Sum(2), Sum(2)]
        for xc in range(XC):
            for yc in range(YC):
                for zc in range(ZC):
                    at = (c, xc, yc, zc)
                    value = fluct[at] + alpha * direction[at]
                    turned[pl.ds(xc * HALF + yc * VOX + zc, 8, stride=3), :] = value
                    for d in range(3):
                        sums[d].add(value * rhs[d, xc, yc, zc])
        for d in range(3):
            entry = total_of(sums[d].get())
            entries[d, c] = ((face_totals[d] - entry) if d == c else -entry) * scale
        for xc in range(XC):
            for t, (start, size) in enumerate(SPANS):
                block = turned[xc * HALF + start : xc * HALF + start + size, :].T
                for xs in range(8):
                    for yh in range(2):
                        row = (xs * 2 + yh) * 8
                        piece = block[row : row + 8]
                        if size < 128:
                            piece = jnp.concatenate([piece, jnp.zeros((8, 128 - size), jnp.float32)], axis=1)
                        rows.at[t][pl.ds(yh * ELEMENTS * VOX + 3 * xs + xc, 8, stride=VOX), :] = piece
        for e in range(ELEMENTS):
            for yh in range(2):
                base = (yh * ELEMENTS + e) * VOX
                for t, (start, size) in enumerate(SPANS):
                    states_ref[0, 0, e, c, :, yh * HALF + start : yh * HALF + start + size] = rows[
                        t, base : base + VOX, 0:size
                    ]


    for d in range(3):
        for c in range(3):
            tangent_ref[0, d, c] = entries[d, c][0:1, 0:ELEMENTS]

    whole = pltpu.make_async_remote_copy(
        src_ref=got.at[pl.ds(0, n - 1)],
        dst_ref=got.at[pl.ds(0, n - 1)],
        send_sem=send_sem,
        recv_sem=recv_sem,
        device_id=peer_of(row, col, offsets[0], nrow, ncol),
        device_id_type=pl.DeviceIdType.MESH,
    )
    whole.wait_recv()
    group = lane >> 3
    for half in range(2):
        found = [jnp.zeros((8, 128), jnp.float32)] * 5
        for c in range(ncol // 2):
            block = got[8 * (half * (ncol // 2) + c) : 8 * (half * (ncol // 2) + c) + 8]
            for f in range(5):
                found[f] = jnp.where(group == (c + f) % 16, block, found[f])
        for f in range(5):
            table_ref[f, half] = found[f]
    whole.wait_send()


def fused(phases, grain, phase_cond, counts, current, load, nrow, ncol):
    field = pltpu.VMEM((3, XC, YC, ZC, 8, 128), jnp.float32)
    vmem = pl.BlockSpec(memory_space=pltpu.VMEM)
    smem = pl.BlockSpec(memory_space=pltpu.SMEM)
    return pl.pallas_call(
        functools.partial(fused_kernel, nrow, ncol),
        out_shape=(
            jax.ShapeDtypeStruct((1, 1, ELEMENTS, 3, VOX, YZ), jnp.float32),
            jax.ShapeDtypeStruct((1, 3, 3, 1, ELEMENTS), jnp.float32),
            jax.ShapeDtypeStruct((5, 2, 8, 128), jnp.float32),
        ),
        in_specs=[vmem, vmem, smem, smem, smem, smem],
        out_specs=(vmem, vmem, vmem),
        scratch_shapes=[
            pltpu.VMEM((3, 2 * ELEMENTS * VOX, 128), jnp.float32),
            pltpu.VMEM((XC * HALF, 128), jnp.float32),
            pltpu.VMEM((XC, YC, ZC, 8, 128), jnp.float32),
            field, field, field, field, field, field,
            pltpu.VMEM((3, 3, 8, 128), jnp.float32),
            pltpu.VMEM((1, 128), jnp.float32),
            pltpu.VMEM((nrow * ncol, 128), jnp.float32),
            pltpu.SemaphoreType.DMA,
            pltpu.SemaphoreType.DMA,
            pltpu.SemaphoreType.DMA,
        ],
        compiler_params=pltpu.CompilerParams(collective_id=0, has_side_effects=True, vmem_limit_bytes=40 * 2**20),
        name="fused",
    )(phases, grain, phase_cond, counts, current, load)


def coarse_kernel(ncol, table_ref, tangent_in, states_in, inc_ref, res_ref, tangent_ref, states_ref, out_sems):
    stores = [pltpu.make_async_copy(states_in.at[0, 0, e], states_ref.at[0, 0, e], out_sems.at[e]) for e in range(ELEMENTS)]
    for copy in stores:
        copy.start()
    tangent_ref[...] = tangent_in[...]

    lane = lax.broadcasted_iota(jnp.int32, (8, 128), 1)
    ex = lax.broadcasted_iota(jnp.int32, (8, 128), 0)
    group, ez = lane >> 3, lane & 7

    def field(f):
        return [pltpu.roll(table_ref[f, h], (128 - 8 * f) % 128, 1) for h in range(2)]

    def x_up(v):
        return [pltpu.roll(part, 7, 0) for part in v]

    def x_down(v):
        return [pltpu.roll(part, 1, 0) for part in v]

    def y_up(v):
        first, second = (pltpu.roll(part, 120, 1) for part in v)
        return [jnp.where(group < 15, first, second), second]

    def y_down(v):
        first, second = (pltpu.roll(part, 8, 1) for part in v)
        return [first, jnp.where(group > 0, second, first)]

    def z_up(v):
        return [pltpu.roll(part, 127, 1) for part in v]

    def z_down(v):
        return [pltpu.roll(part, 1, 1) for part in v]

    yes = ex >= 0
    moves = (
        (0, x_up, [ex < 7] * 2), (0, x_down, [ex > 0] * 2),
        (1, y_up, [yes, group < 15]), (1, y_down, [group > 0, yes]),
        (2, z_up, [ez < 7] * 2), (2, z_down, [ez > 0] * 2),
    )
    centre = [jnp.zeros((8, 128), jnp.float32)] * 2
    weights = []
    kd = [field(d) for d in range(3)]
    for d, move, has in moves:
        other = move(kd[d])
        pair = [0.5 * (own + jnp.where(ok, far, 0.0)) for own, far, ok in zip(kd[d], other, has)]
        centre = [c + p for c, p in zip(centre, pair)]
        weights.append([jnp.where(ok, p, 0.0) for p, ok in zip(pair, has)])

    def apply(v):
        moved = [move(v) for _, move, _ in moves]
        out = []
        for h in range(2):
            parts = [weights[i][h] * moved[i][h] for i in range(6)]
            out.append(centre[h] * v[h] - ((parts[0] + parts[1]) + (parts[2] + parts[3]) + (parts[4] + parts[5])))
        return out

    def total(u, v):
        value = u[0] * v[0] + u[1] * v[1]
        for shift in (1, 2, 4):
            value = value + pltpu.roll(value, shift, 0)
        return jnp.sum(value, axis=1, keepdims=True)

    def axpy(a, u, v):
        return [a * p + q for p, q in zip(u, v)]

    image = apply(field(3))
    residual = [p - q for p, q in zip(field(4), image)]
    image = apply(residual)
    increment = older = alpha = None
    for i in range(MACRO_ITERS):
        gamma, delta = total(residual, residual), total(image, residual)
        deep = apply(image) if i < MACRO_ITERS - 1 else None
        if i == 0:
            alpha = gamma / delta
            p, s, z = residual, image, deep
            increment = [alpha * v for v in p]
        else:
            beta = gamma / older
            alpha = gamma / (delta - beta * gamma / alpha)
            p, s = axpy(beta, p, residual), axpy(beta, s, image)
            z = axpy(beta, z, deep) if deep is not None else None
            increment = axpy(alpha, p, increment)
        older = gamma
        residual = axpy(-alpha, s, residual)
        if deep is not None:
            image = axpy(-alpha, z, image)

    row, col = lax.axis_index("row"), lax.axis_index("col")
    for value, ref in ((increment, inc_ref), (residual, res_ref)):
        own = jnp.where(ex == row, jnp.where(col < 16, value[0], value[1]), 0.0)
        own = jnp.where(group == (col & 15), own, 0.0)
        for shift in (1, 2, 4):
            own = own + pltpu.roll(own, shift, 0)
        own = pltpu.roll(own, (128 - 8 * (col & 15)) & 127, 1)
        ref[0] = own[0:1, 0:ELEMENTS]
    for outgoing in stores:
        outgoing.wait()


def coarse(table, tangent, states, ncol):
    vmem = pl.BlockSpec(memory_space=pltpu.VMEM)
    anywhere = pl.BlockSpec(memory_space=pl.ANY)
    small = jax.ShapeDtypeStruct((1, 1, ELEMENTS), jnp.float32)
    return pl.pallas_call(
        functools.partial(coarse_kernel, ncol),
        out_shape=(
            small, small,
            jax.ShapeDtypeStruct(tangent.shape, jnp.float32),
            jax.ShapeDtypeStruct(states.shape, jnp.float32),
        ),
        in_specs=[vmem, vmem, anywhere],
        out_specs=(vmem, vmem, vmem, anywhere),
        scratch_shapes=[
            pltpu.SemaphoreType.DMA((ELEMENTS,)),
        ],
        compiler_params=pltpu.CompilerParams(vmem_limit_bytes=16 * 2**20),
        name="coarse",
    )(table, tangent, states)


def shards(nrow, ncol, phases, grain, phase_cond, micro_counts, current, load):
    states, tangent, table = fused(phases, grain, phase_cond, micro_counts, current, load, nrow, ncol)
    increment, residual, tangent, states = coarse(table, tangent, states, ncol)
    return (states, tangent.transpose(0, 3, 4, 1, 2), increment, residual)


def solution(mesh):
    placed = (
        P("row", "col", None, None, None),
        P("row", "col", None, None, None),
        P(),
        P("row", "col", None),
        P("row", "col", None),
        P("row", "col", None),
    )
    return jax.shard_map(
        functools.partial(shards, mesh.shape["row"], mesh.shape["col"]),
        mesh=mesh,
        in_specs=placed,
        out_specs=(
            P("row", "col", None, None, None, None),
            P("row", "col", None, None, None),
            P("row", "col", None),
            P("row", "col", None),
        ),
        check_vma=False,
    )
```

```python
import functools

import jax
import jax.numpy as jnp
from jax import lax
from jax.experimental import pallas as pl
from jax.experimental.pallas import tpu as pltpu
from jax.sharding import PartitionSpec as P

VOX = 24
YZ = 576
PHASES = 3
MACRO_ITERS = 8
MICRO_MAX = 12

XC, YC, ZC = 3, 12, 3
ELEMENTS = 8
HALF = YZ // 2
SPANS = ((0, 128), (128, 128), (256, 32))


def swap_half(value):
    lane = lax.broadcasted_iota(jnp.int32, value.shape, 1)
    return jnp.where((lane & 8) == 0, pltpu.roll(value, 120, 1), pltpu.roll(value, 8, 1))


def next_x(value):
    return pltpu.roll(value, 112, 1)


def prev_x(value):
    return pltpu.roll(value, 16, 1)


def next_z(value):
    return pltpu.roll(value, 7, 0)


def prev_z(value):
    return pltpu.roll(value, 1, 0)


def total_of(value):
    for shift in (1, 2, 4):
        value = value + pltpu.roll(value, shift, 0)
    k = lax.broadcasted_iota(jnp.int32, (128, 128), 0)
    j = lax.broadcasted_iota(jnp.int32, (128, 128), 1)
    same = jnp.where((k & 7) == (j & 7), 1.0, 0.0)
    return jnp.dot(value, same, precision=lax.Precision.HIGHEST, preferred_element_type=jnp.float32)


SPOTS = [(xc, zc) for xc in range(XC) for zc in range(ZC)]


def plane(ref, yc, lead=()):
    return {(xc, zc): ref[(*lead, xc, yc, zc)] for xc, zc in SPOTS}


def ahead_x(values, xc, zc):
    return values[xc + 1, zc] if xc < XC - 1 else next_x(values[0, zc])


def back_x(values, xc, zc, wrap=None):
    if wrap is not None and xc == 0:
        return wrap[zc]
    return values[xc - 1, zc] if xc > 0 else prev_x(values[XC - 1, zc])


def ahead_z(values, xc, zc):
    return values[xc, zc + 1] if zc < ZC - 1 else next_z(values[xc, 0])


def back_z(values, xc, zc):
    return values[xc, zc - 1] if zc > 0 else prev_z(values[xc, ZC - 1])


def swapped(values):
    return {spot: swap_half(value) for spot, value in values.items()}


class Sum:
    def __init__(self, ways=4):
        self.parts = [None] * ways
        self.at = 0

    def add(self, value):
        slot = self.at % len(self.parts)
        self.at += 1
        self.parts[slot] = value if self.parts[slot] is None else self.parts[slot] + value

    def get(self):
        parts = [part for part in self.parts if part is not None]
        while len(parts) > 1:
            parts = [sum(parts[i : i + 2][1:], parts[i]) for i in range(0, len(parts), 2)]
        return parts[0]


def far_first(nrow, ncol):
    ny, nx = nrow // 2, 4
    nz = ncol // nx
    offsets = [
        (y, core, x, z) for y in range(ny) for core in range(2) for x in range(nx) for z in range(nz)
    ]

    def hops(offset):
        y, core, x, z = offset
        return min(y, ny - y) + min(x, nx - x) + min(z, nz - z) + 0.5 * core

    return sorted(offsets[1:], key=hops, reverse=True)


def peer_of(row, col, offset, nrow, ncol):
    ny, nx = nrow // 2, 4
    nz = ncol // nx
    y, core, x, z = offset
    return {
        "row": lax.rem(row // 2 + y, ny) * 2 + lax.rem(row + core, 2),
        "col": lax.rem(col // nz + x, nx) * nz + lax.rem(lax.rem(col, nz) + z, nz),
    }


def fused_kernel(
    nrow, ncol,
    phases_in, grain_in, pc_in, counts_in, current_in, load_in, states_ref, tangent_ref, table_ref,
    phases_ref, grain_ref, pc_ref, counts_ref, current_ref, load_ref, in_sems, back_faces, placed, out_sems,
    rows, turned, cond, faces, rhs, fluct, remain, direction, image, scal, mine, got, send_sem, recv_sem,
):
    n = nrow * ncol
    row, col = lax.axis_index("row"), lax.axis_index("col")
    smalls = [
        pltpu.make_async_copy(source, target, in_sems.at[ELEMENTS + i])
        for i, (source, target) in enumerate(
            ((pc_in, pc_ref), (counts_in, counts_ref), (current_in, current_ref), (load_in, load_ref))
        )
    ]
    voxels = [
        [
            pltpu.make_async_copy(source.at[0, 0, e], target.at[0, 0, e], in_sems.at[e])
            for source, target in ((phases_in, phases_ref), (grain_in, grain_ref))
        ]
        for e in range(ELEMENTS)
    ]
    for copy in smalls + sum(voxels, []):
        copy.start()
    offsets = far_first(nrow, ncol)
    barrier = pltpu.get_barrier_semaphore()
    for offset in offsets:
        pl.semaphore_signal(
            barrier, inc=1, device_id=peer_of(row, col, offset, nrow, ncol), device_id_type=pl.DeviceIdType.MESH
        )

    for copy in smalls:
        copy.wait()
    pc = [pc_ref[k] for k in range(PHASES)]
    for e in range(ELEMENTS):
        for copy in voxels[e]:
            copy.wait()
        phase = phases_ref[0, 0, e]
        value = jnp.where(phase == 0, pc[0], jnp.where(phase == 1, pc[1], pc[2])) * grain_ref[0, 0, e]
        for yh in range(2):
            base = (yh * ELEMENTS + e) * VOX
            for t, (start, size) in enumerate(SPANS):
                rows[t, base : base + VOX, 0:size] = value[:, yh * HALF + start : yh * HALF + start + size]
    for xc in range(XC):
        for t, (start, size) in enumerate(SPANS):
            parts = []
            for xs in range(8):
                for yh in range(2):
                    parts.append(rows.at[t][pl.ds(yh * ELEMENTS * VOX + 3 * xs + xc, 8, stride=VOX), :])
            block = jnp.concatenate(parts, axis=0).T
            turned[xc * HALF + start : xc * HALF + start + size, :] = block[0:size]
    for xc in range(XC):
        for yc in range(YC):
            for zc in range(ZC):
                cond[xc, yc, zc] = turned[pl.ds(xc * HALF + yc * VOX + zc, 8, stride=3), :]

    face_sums = [Sum(), Sum(), Sum()]
    here = plane(cond, 0)
    for yc in range(YC):
        ahead = plane(cond, yc + 1) if yc < YC - 1 else swapped(plane(cond, 0))
        for xc, zc in SPOTS:
            own = here[xc, zc]
            for d, other in enumerate((ahead_x(here, xc, zc), ahead[xc, zc], ahead_z(here, xc, zc))):
                face = (own + other) * 0.5
                faces[d, xc, yc, zc] = face
                face_sums[d].add(face)
        here = ahead
    norms = [Sum(), Sum(), Sum()]
    before = swapped(plane(faces, YC - 1, (1,)))
    for yc in range(YC):
        fx, fy, fz = (plane(faces, yc, (d,)) for d in range(3))
        for xc, zc in SPOTS:
            backs = (back_x(fx, xc, zc), before[xc, zc], back_z(fz, xc, zc))
            for d, own in enumerate((fx[xc, zc], fy[xc, zc], fz[xc, zc])):
                value = own - backs[d]
                rhs[d, xc, yc, zc] = value
                if d == 0 and xc == 0:
                    back_faces[yc, zc] = backs[0]
                remain[d, xc, yc, zc] = value
                norms[d].add(value * value)
        before = fy

    lane = lax.broadcasted_iota(jnp.int32, (8, 128), 1)
    counts = jnp.zeros((8, 128), jnp.int32)
    coarse = [jnp.zeros((8, 128), jnp.float32)] * 2
    for e in range(ELEMENTS):
        here_e = (lane & 7) == e
        counts = jnp.where(here_e, counts_ref[0, 0, e], counts)
        coarse = [jnp.where(here_e, ref[0, 0, e], value) for ref, value in zip((current_ref, load_ref), coarse)]

    def sweep(c, alpha, beta, first):
        curv = Sum()

        def fresh(yc):
            out = {}
            for xc, zc in SPOTS:
                at = (c, xc, yc, zc)
                if first:
                    value = remain[at]
                    fluct[at] = jnp.zeros((8, 128), jnp.float32)
                else:
                    old = direction[at]
                    fluct[at] = fluct[at] + alpha * old
                    value = remain[at] + beta * old
                direction[at] = value
                out[xc, zc] = value
            return out

        last = fresh(YC - 1)
        here = fresh(0)
        flow_back = {
            s: swap_half(faces[1, s[0], YC - 1, s[1]] * (last[s] - swap_half(here[s]))) for s in SPOTS
        }
        for yc in range(YC):
            if yc < YC - 2:
                ahead = fresh(yc + 1)
            elif yc == YC - 2:
                ahead = plane(direction, YC - 1, (c,))
            else:
                ahead = swapped(plane(direction, 0, (c,)))
            gx, gy, gz = {}, {}, {}
            for xc, zc in SPOTS:
                own = here[xc, zc]
                gx[xc, zc] = faces[0, xc, yc, zc] * (own - ahead_x(here, xc, zc))
                gy[xc, zc] = faces[1, xc, yc, zc] * (own - ahead[xc, zc])
                gz[xc, zc] = faces[2, xc, yc, zc] * (own - ahead_z(here, xc, zc))
            wrap = [back_faces[yc, zc] * (prev_x(here[XC - 1, zc]) - here[0, zc]) for zc in range(ZC)]
            for xc, zc in SPOTS:
                value = (
                    (gx[xc, zc] - back_x(gx, xc, zc, wrap))
                    + (gy[xc, zc] - flow_back[xc, zc])
                    + (gz[xc, zc] - back_z(gz, xc, zc))
                )
                image[c, xc, yc, zc] = value
                curv.add(here[xc, zc] * value)
            flow_back = gy
            here = ahead
        return total_of(curv.get())

    def reduce_residual(c, alpha):
        norm = Sum()
        for yc in range(YC):
            for xc, zc in SPOTS:
                at = (c, xc, yc, zc)
                value = remain[at] - alpha * image[at]
                remain[at] = value
                norm.add(value * value)
        return total_of(norm.get())

    for c in range(3):
        norm = total_of(norms[c].get())
        curv = sweep(c, None, None, True)
        scal[0, c] = norm
        alpha = norm / curv
        scal[1, c] = alpha
        scal[2, c] = alpha * norm

    def iterate(index, carry):
        for c in range(3):
            alpha = scal[1, c]
            norm = scal[0, c]
            norm_next = reduce_residual(c, alpha)
            active = index < counts
            curv = sweep(c, alpha, jnp.where(active, norm_next / norm, 0.0), False)
            scal[0, c] = norm_next
            alpha = jnp.where(active, norm_next / curv, 0.0)
            scal[1, c] = alpha
            scal[2, c] = scal[2, c] + alpha * norm_next
        return carry

    lax.fori_loop(1, MICRO_MAX, iterate, 0)

    scale = 1.0 / (VOX * YZ)
    face_totals = [total_of(part.get()) for part in face_sums]
    fields = [(face_totals[d] - scal[2, d]) * scale for d in range(3)] + coarse
    slot = ((lane >> 3) - col) & 15
    packed = fields[4]
    for f in range(4):
        packed = jnp.where(slot == f, fields[f], packed)
    mine[...] = packed[0:1]

    me = col * nrow + row
    pl.semaphore_wait(barrier, n - 1)
    got[pl.ds(me, 1)] = packed[0:1]
    for offset in offsets:
        pltpu.make_async_remote_copy(
            src_ref=mine,
            dst_ref=got.at[pl.ds(me, 1)],
            send_sem=send_sem,
            recv_sem=recv_sem,
            device_id=peer_of(row, col, offset, nrow, ncol),
            device_id_type=pl.DeviceIdType.MESH,
        ).start()

    entries = {}
    for c in range(3):
        alpha = scal[1, c]
        sums = [Sum(2), Sum(2), Sum(2)]
        for xc in range(XC):
            for yc in range(YC):
                for zc in range(ZC):
                    at = (c, xc, yc, zc)
                    value = fluct[at] + alpha * direction[at]
                    turned[pl.ds(xc * HALF + yc * VOX + zc, 8, stride=3), :] = value
                    for d in range(3):
                        sums[d].add(value * rhs[d, xc, yc, zc])
        for d in range(3):
            entry = total_of(sums[d].get())
            entries[d, c] = ((face_totals[d] - entry) if d == c else -entry) * scale
        for xc in range(XC):
            for t, (start, size) in enumerate(SPANS):
                block = turned[xc * HALF + start : xc * HALF + start + size, :].T
                for xs in range(8):
                    for yh in range(2):
                        row = (xs * 2 + yh) * 8
                        piece = block[row : row + 8]
                        if size < 128:
                            piece = jnp.concatenate([piece, jnp.zeros((8, 128 - size), jnp.float32)], axis=1)
                        rows.at[t][pl.ds(yh * ELEMENTS * VOX + 3 * xs + xc, 8, stride=VOX), :] = piece
        for e in range(ELEMENTS):
            for yh in range(2):
                base = (yh * ELEMENTS + e) * VOX
                for t, (start, size) in enumerate(SPANS):
                    placed[e, c, :, yh * HALF + start : yh * HALF + start + size] = rows[
                        t, base : base + VOX, 0:size
                    ]


    for d in range(3):
        for c in range(3):
            tangent_ref[0, d, c] = entries[d, c][0:1, 0:ELEMENTS]

    stores = [pltpu.make_async_copy(placed.at[e], states_ref.at[0, 0, e], out_sems.at[e]) for e in range(ELEMENTS)]
    for copy in stores:
        copy.start()

    whole = pltpu.make_async_remote_copy(
        src_ref=got.at[pl.ds(0, n - 1)],
        dst_ref=got.at[pl.ds(0, n - 1)],
        send_sem=send_sem,
        recv_sem=recv_sem,
        device_id=peer_of(row, col, offsets[0], nrow, ncol),
        device_id_type=pl.DeviceIdType.MESH,
    )
    whole.wait_recv()
    group = lane >> 3
    for half in range(2):
        found = [jnp.zeros((8, 128), jnp.float32)] * 5
        for c in range(ncol // 2):
            block = got[8 * (half * (ncol // 2) + c) : 8 * (half * (ncol // 2) + c) + 8]
            for f in range(5):
                found[f] = jnp.where(group == (c + f) % 16, block, found[f])
        for f in range(5):
            table_ref[f, half] = found[f]
    whole.wait_send()
    for copy in stores:
        copy.wait()


def fused(phases, grain, phase_cond, counts, current, load, nrow, ncol):
    field = pltpu.VMEM((3, XC, YC, ZC, 8, 128), jnp.float32)
    vmem = pl.BlockSpec(memory_space=pltpu.VMEM)
    return pl.pallas_call(
        functools.partial(fused_kernel, nrow, ncol),
        out_shape=(
            jax.ShapeDtypeStruct((1, 1, ELEMENTS, 3, VOX, YZ), jnp.float32),
            jax.ShapeDtypeStruct((1, 3, 3, 1, ELEMENTS), jnp.float32),
            jax.ShapeDtypeStruct((5, 2, 8, 128), jnp.float32),
        ),
        in_specs=[pl.BlockSpec(memory_space=pltpu.HBM)] * 6,
        out_specs=(pl.BlockSpec(memory_space=pltpu.HBM), vmem, vmem),
        scratch_shapes=[
            pltpu.VMEM(phases.shape, jnp.int32),
            pltpu.VMEM(grain.shape, jnp.float32),
            pltpu.SMEM(phase_cond.shape, jnp.float32),
            pltpu.SMEM(counts.shape, jnp.int32),
            pltpu.SMEM(current.shape, jnp.float32),
            pltpu.SMEM(load.shape, jnp.float32),
            pltpu.SemaphoreType.DMA((ELEMENTS + 4,)),
            pltpu.VMEM((YC, ZC, 8, 128), jnp.float32),
            pltpu.VMEM((ELEMENTS, 3, VOX, YZ), jnp.float32),
            pltpu.SemaphoreType.DMA((ELEMENTS,)),
            pltpu.VMEM((3, 2 * ELEMENTS * VOX, 128), jnp.float32),
            pltpu.VMEM((XC * HALF, 128), jnp.float32),
            pltpu.VMEM((XC, YC, ZC, 8, 128), jnp.float32),
            field, field, field, field, field, field,
            pltpu.VMEM((3, 3, 8, 128), jnp.float32),
            pltpu.VMEM((1, 128), jnp.float32),
            pltpu.VMEM((nrow * ncol, 128), jnp.float32),
            pltpu.SemaphoreType.DMA,
            pltpu.SemaphoreType.DMA,
        ],
        compiler_params=pltpu.CompilerParams(collective_id=0, has_side_effects=True),
        name="fused",
    )(phases, grain, phase_cond, counts, current, load)


def coarse_kernel(ncol, table_ref, tangent_in, states_in, inc_ref, res_ref, tangent_ref, states_ref, held, in_sems, out_sems):
    loads = [pltpu.make_async_copy(states_in.at[0, 0, e], held.at[e], in_sems.at[e]) for e in range(ELEMENTS)]
    stores = [pltpu.make_async_copy(held.at[e], states_ref.at[0, 0, e], out_sems.at[e]) for e in range(ELEMENTS)]
    for copy in loads:
        copy.start()
    tangent_ref[...] = tangent_in[...]

    lane = lax.broadcasted_iota(jnp.int32, (8, 128), 1)
    ex = lax.broadcasted_iota(jnp.int32, (8, 128), 0)
    group, ez = lane >> 3, lane & 7

    def field(f):
        return [pltpu.roll(table_ref[f, h], (128 - 8 * f) % 128, 1) for h in range(2)]

    def x_up(v):
        return [pltpu.roll(part, 7, 0) for part in v]

    def x_down(v):
        return [pltpu.roll(part, 1, 0) for part in v]

    def y_up(v):
        first, second = (pltpu.roll(part, 120, 1) for part in v)
        return [jnp.where(group < 15, first, second), second]

    def y_down(v):
        first, second = (pltpu.roll(part, 8, 1) for part in v)
        return [first, jnp.where(group > 0, second, first)]

    def z_up(v):
        return [pltpu.roll(part, 127, 1) for part in v]

    def z_down(v):
        return [pltpu.roll(part, 1, 1) for part in v]

    yes = ex >= 0
    moves = (
        (0, x_up, [ex < 7] * 2), (0, x_down, [ex > 0] * 2),
        (1, y_up, [yes, group < 15]), (1, y_down, [group > 0, yes]),
        (2, z_up, [ez < 7] * 2), (2, z_down, [ez > 0] * 2),
    )
    centre = [jnp.zeros((8, 128), jnp.float32)] * 2
    weights = []
    kd = [field(d) for d in range(3)]
    for d, move, has in moves:
        other = move(kd[d])
        pair = [0.5 * (own + jnp.where(ok, far, 0.0)) for own, far, ok in zip(kd[d], other, has)]
        centre = [c + p for c, p in zip(centre, pair)]
        weights.append([jnp.where(ok, p, 0.0) for p, ok in zip(pair, has)])

    def apply(v):
        moved = [move(v) for _, move, _ in moves]
        out = []
        for h in range(2):
            parts = [weights[i][h] * moved[i][h] for i in range(6)]
            out.append(centre[h] * v[h] - ((parts[0] + parts[1]) + (parts[2] + parts[3]) + (parts[4] + parts[5])))
        return out

    def total(u, v):
        value = u[0] * v[0] + u[1] * v[1]
        for shift in (1, 2, 4):
            value = value + pltpu.roll(value, shift, 0)
        return jnp.sum(value, axis=1, keepdims=True)

    def axpy(a, u, v):
        return [a * p + q for p, q in zip(u, v)]

    image = apply(field(3))
    residual = [p - q for p, q in zip(field(4), image)]
    image = apply(residual)
    increment = older = alpha = None
    for i in range(MACRO_ITERS):
        gamma, delta = total(residual, residual), total(image, residual)
        deep = apply(image) if i < MACRO_ITERS - 1 else None
        if i == 0:
            alpha = gamma / delta
            p, s, z = residual, image, deep
            increment = [alpha * v for v in p]
        else:
            beta = gamma / older
            alpha = gamma / (delta - beta * gamma / alpha)
            p, s = axpy(beta, p, residual), axpy(beta, s, image)
            z = axpy(beta, z, deep) if deep is not None else None
            increment = axpy(alpha, p, increment)
        older = gamma
        residual = axpy(-alpha, s, residual)
        if deep is not None:
            image = axpy(-alpha, z, image)
        if i == 1:
            for incoming, outgoing in zip(loads, stores):
                incoming.wait()
                outgoing.start()

    row, col = lax.axis_index("row"), lax.axis_index("col")
    for value, ref in ((increment, inc_ref), (residual, res_ref)):
        own = jnp.where(ex == row, jnp.where(col < 16, value[0], value[1]), 0.0)
        own = jnp.where(group == (col & 15), own, 0.0)
        for shift in (1, 2, 4):
            own = own + pltpu.roll(own, shift, 0)
        own = pltpu.roll(own, (128 - 8 * (col & 15)) & 127, 1)
        ref[0] = own[0:1, 0:ELEMENTS]
    for outgoing in stores:
        outgoing.wait()


def coarse(table, tangent, states, ncol):
    vmem = pl.BlockSpec(memory_space=pltpu.VMEM)
    anywhere = pl.BlockSpec(memory_space=pl.ANY)
    small = jax.ShapeDtypeStruct((1, 1, ELEMENTS), jnp.float32)
    return pl.pallas_call(
        functools.partial(coarse_kernel, ncol),
        out_shape=(
            small, small,
            jax.ShapeDtypeStruct(tangent.shape, jnp.float32),
            jax.ShapeDtypeStruct(states.shape, jnp.float32),
        ),
        in_specs=[vmem, vmem, anywhere],
        out_specs=(vmem, vmem, vmem, anywhere),
        scratch_shapes=[
            pltpu.VMEM((ELEMENTS, 3, VOX, YZ), jnp.float32),
            pltpu.SemaphoreType.DMA((ELEMENTS,)),
            pltpu.SemaphoreType.DMA((ELEMENTS,)),
        ],
        name="coarse",
    )(table, tangent, states)


def shards(nrow, ncol, phases, grain, phase_cond, micro_counts, current, load):
    states, tangent, table = fused(phases, grain, phase_cond, micro_counts, current, load, nrow, ncol)
    increment, residual, tangent, states = coarse(table, tangent, states, ncol)
    return (states, tangent.transpose(0, 3, 4, 1, 2), increment, residual)


def solution(mesh):
    placed = (
        P("row", "col", None, None, None),
        P("row", "col", None, None, None),
        P(),
        P("row", "col", None),
        P("row", "col", None),
        P("row", "col", None),
    )
    return jax.shard_map(
        functools.partial(shards, mesh.shape["row"], mesh.shape["col"]),
        mesh=mesh,
        in_specs=placed,
        out_specs=(
            P("row", "col", None, None, None, None),
            P("row", "col", None, None, None),
            P("row", "col", None),
            P("row", "col", None),
        ),
        check_vma=False,
    )
```

```python
import functools

import jax
import jax.numpy as jnp
from jax import lax
from jax.experimental import pallas as pl
from jax.experimental.pallas import tpu as pltpu
from jax.sharding import PartitionSpec as P

VOX = 24
YZ = 576
PHASES = 3
MACRO_ITERS = 8
MICRO_MAX = 12

XC, YC, ZC = 3, 12, 3
ELEMENTS = 8
HALF = YZ // 2
SPANS = ((0, 128), (128, 128), (256, 32))


def swap_half(value):
    lane = lax.broadcasted_iota(jnp.int32, value.shape, 1)
    return jnp.where((lane & 8) == 0, pltpu.roll(value, 120, 1), pltpu.roll(value, 8, 1))


def next_x(value):
    return pltpu.roll(value, 112, 1)


def prev_x(value):
    return pltpu.roll(value, 16, 1)


def next_z(value):
    return pltpu.roll(value, 7, 0)


def prev_z(value):
    return pltpu.roll(value, 1, 0)


def total_of(value):
    for shift in (1, 2, 4):
        value = value + pltpu.roll(value, shift, 0)
    k = lax.broadcasted_iota(jnp.int32, (128, 128), 0)
    j = lax.broadcasted_iota(jnp.int32, (128, 128), 1)
    same = jnp.where((k & 7) == (j & 7), 1.0, 0.0).astype(jnp.bfloat16)
    first = value.astype(jnp.bfloat16)
    rest = value - first.astype(jnp.float32)
    second = rest.astype(jnp.bfloat16)
    third = (rest - second.astype(jnp.float32)).astype(jnp.bfloat16)
    parts = [jnp.dot(part, same, preferred_element_type=jnp.float32) for part in (first, second, third)]
    return parts[0] + (parts[1] + parts[2])


SPOTS = [(xc, zc) for xc in range(XC) for zc in range(ZC)]


def plane(ref, yc, lead=()):
    return {(xc, zc): ref[(*lead, xc, yc, zc)] for xc, zc in SPOTS}


def ahead_x(values, xc, zc):
    return values[xc + 1, zc] if xc < XC - 1 else next_x(values[0, zc])


def back_x(values, xc, zc, wrap=None):
    if wrap is not None and xc == 0:
        return wrap[zc]
    return values[xc - 1, zc] if xc > 0 else prev_x(values[XC - 1, zc])


def ahead_z(values, xc, zc):
    return values[xc, zc + 1] if zc < ZC - 1 else next_z(values[xc, 0])


def back_z(values, xc, zc):
    return values[xc, zc - 1] if zc > 0 else prev_z(values[xc, ZC - 1])


def swapped(values):
    return {spot: swap_half(value) for spot, value in values.items()}


class Sum:
    def __init__(self, ways=4):
        self.parts = [None] * ways
        self.at = 0

    def add(self, value):
        slot = self.at % len(self.parts)
        self.at += 1
        self.parts[slot] = value if self.parts[slot] is None else self.parts[slot] + value

    def get(self):
        parts = [part for part in self.parts if part is not None]
        while len(parts) > 1:
            parts = [sum(parts[i : i + 2][1:], parts[i]) for i in range(0, len(parts), 2)]
        return parts[0]


def far_first(nrow, ncol):
    ny, nx = nrow // 2, 4
    nz = ncol // nx
    offsets = [
        (y, core, x, z) for y in range(ny) for core in range(2) for x in range(nx) for z in range(nz)
    ]

    def hops(offset):
        y, core, x, z = offset
        return min(y, ny - y) + min(x, nx - x) + min(z, nz - z) + 0.5 * core

    return sorted(offsets[1:], key=hops, reverse=True)


def peer_of(row, col, offset, nrow, ncol):
    ny, nx = nrow // 2, 4
    nz = ncol // nx
    y, core, x, z = offset
    return {
        "row": lax.rem(row // 2 + y, ny) * 2 + lax.rem(row + core, 2),
        "col": lax.rem(col // nz + x, nx) * nz + lax.rem(lax.rem(col, nz) + z, nz),
    }


def fused_kernel(
    nrow, ncol,
    phases_in, grain_in, pc_in, counts_in, current_in, load_in, states_ref, tangent_ref, table_ref,
    phases_ref, grain_ref, pc_ref, counts_ref, current_ref, load_ref, in_sems, back_faces, placed, out_sems,
    rows, turned, cond, faces, rhs, fluct, remain, direction, image, scal, mine, got, send_sem, recv_sem,
):
    n = nrow * ncol
    row, col = lax.axis_index("row"), lax.axis_index("col")
    smalls = [
        pltpu.make_async_copy(source, target, in_sems.at[ELEMENTS + i])
        for i, (source, target) in enumerate(
            ((pc_in, pc_ref), (counts_in, counts_ref), (current_in, current_ref), (load_in, load_ref))
        )
    ]
    voxels = [
        [
            pltpu.make_async_copy(source.at[0, 0, e], target.at[0, 0, e], in_sems.at[e])
            for source, target in ((phases_in, phases_ref), (grain_in, grain_ref))
        ]
        for e in range(ELEMENTS)
    ]
    for copy in smalls + sum(voxels, []):
        copy.start()
    offsets = far_first(nrow, ncol)
    barrier = pltpu.get_barrier_semaphore()
    for offset in offsets:
        pl.semaphore_signal(
            barrier, inc=1, device_id=peer_of(row, col, offset, nrow, ncol), device_id_type=pl.DeviceIdType.MESH
        )

    for copy in smalls:
        copy.wait()
    pc = [pc_ref[k] for k in range(PHASES)]
    for e in range(ELEMENTS):
        for copy in voxels[e]:
            copy.wait()
        phase = phases_ref[0, 0, e]
        value = jnp.where(phase == 0, pc[0], jnp.where(phase == 1, pc[1], pc[2])) * grain_ref[0, 0, e]
        for yh in range(2):
            base = (yh * ELEMENTS + e) * VOX
            for t, (start, size) in enumerate(SPANS):
                rows[t, base : base + VOX, 0:size] = value[:, yh * HALF + start : yh * HALF + start + size]
    for xc in range(XC):
        for t, (start, size) in enumerate(SPANS):
            parts = []
            for xs in range(8):
                for yh in range(2):
                    parts.append(rows.at[t][pl.ds(yh * ELEMENTS * VOX + 3 * xs + xc, 8, stride=VOX), :])
            block = jnp.concatenate(parts, axis=0).T
            turned[xc * HALF + start : xc * HALF + start + size, :] = block[0:size]
    for xc in range(XC):
        for yc in range(YC):
            for zc in range(ZC):
                cond[xc, yc, zc] = turned[pl.ds(xc * HALF + yc * VOX + zc, 8, stride=3), :]

    face_sums = [Sum(), Sum(), Sum()]
    here = plane(cond, 0)
    for yc in range(YC):
        ahead = plane(cond, yc + 1) if yc < YC - 1 else swapped(plane(cond, 0))
        for xc, zc in SPOTS:
            own = here[xc, zc]
            for d, other in enumerate((ahead_x(here, xc, zc), ahead[xc, zc], ahead_z(here, xc, zc))):
                face = (own + other) * 0.5
                faces[d, xc, yc, zc] = face
                face_sums[d].add(face)
        here = ahead
    norms = [Sum(), Sum(), Sum()]
    before = swapped(plane(faces, YC - 1, (1,)))
    for yc in range(YC):
        fx, fy, fz = (plane(faces, yc, (d,)) for d in range(3))
        for xc, zc in SPOTS:
            backs = (back_x(fx, xc, zc), before[xc, zc], back_z(fz, xc, zc))
            for d, own in enumerate((fx[xc, zc], fy[xc, zc], fz[xc, zc])):
                value = own - backs[d]
                rhs[d, xc, yc, zc] = value
                if d == 0 and xc == 0:
                    back_faces[yc, zc] = backs[0]
                remain[d, xc, yc, zc] = value
                norms[d].add(value * value)
        before = fy

    lane = lax.broadcasted_iota(jnp.int32, (8, 128), 1)
    counts = jnp.zeros((8, 128), jnp.int32)
    coarse = [jnp.zeros((8, 128), jnp.float32)] * 2
    for e in range(ELEMENTS):
        here_e = (lane & 7) == e
        counts = jnp.where(here_e, counts_ref[0, 0, e], counts)
        coarse = [jnp.where(here_e, ref[0, 0, e], value) for ref, value in zip((current_ref, load_ref), coarse)]

    def sweep(c, alpha, beta, first):
        curv = Sum()

        def fresh(yc):
            out = {}
            for xc, zc in SPOTS:
                at = (c, xc, yc, zc)
                if first:
                    value = remain[at]
                    fluct[at] = jnp.zeros((8, 128), jnp.float32)
                else:
                    old = direction[at]
                    fluct[at] = fluct[at] + alpha * old
                    value = remain[at] + beta * old
                direction[at] = value
                out[xc, zc] = value
            return out

        last = fresh(YC - 1)
        here = fresh(0)
        flow_back = {
            s: swap_half(faces[1, s[0], YC - 1, s[1]] * (last[s] - swap_half(here[s]))) for s in SPOTS
        }
        for yc in range(YC):
            if yc < YC - 2:
                ahead = fresh(yc + 1)
            elif yc == YC - 2:
                ahead = plane(direction, YC - 1, (c,))
            else:
                ahead = swapped(plane(direction, 0, (c,)))
            gx, gy, gz = {}, {}, {}
            for xc, zc in SPOTS:
                own = here[xc, zc]
                gx[xc, zc] = faces[0, xc, yc, zc] * (own - ahead_x(here, xc, zc))
                gy[xc, zc] = faces[1, xc, yc, zc] * (own - ahead[xc, zc])
                gz[xc, zc] = faces[2, xc, yc, zc] * (own - ahead_z(here, xc, zc))
            wrap = [back_faces[yc, zc] * (prev_x(here[XC - 1, zc]) - here[0, zc]) for zc in range(ZC)]
            for xc, zc in SPOTS:
                value = (
                    (gx[xc, zc] - back_x(gx, xc, zc, wrap))
                    + (gy[xc, zc] - flow_back[xc, zc])
                    + (gz[xc, zc] - back_z(gz, xc, zc))
                )
                image[c, xc, yc, zc] = value
                curv.add(here[xc, zc] * value)
            flow_back = gy
            here = ahead
        return total_of(curv.get())

    def reduce_residual(c, alpha):
        norm = Sum()
        for yc in range(YC):
            for xc, zc in SPOTS:
                at = (c, xc, yc, zc)
                value = remain[at] - alpha * image[at]
                remain[at] = value
                norm.add(value * value)
        return total_of(norm.get())

    for c in range(3):
        norm = total_of(norms[c].get())
        curv = sweep(c, None, None, True)
        scal[0, c] = norm
        alpha = norm / curv
        scal[1, c] = alpha
        scal[2, c] = alpha * norm

    def iterate(index, carry):
        for c in range(3):
            alpha = scal[1, c]
            norm = scal[0, c]
            norm_next = reduce_residual(c, alpha)
            active = index < counts
            curv = sweep(c, alpha, jnp.where(active, norm_next / norm, 0.0), False)
            scal[0, c] = norm_next
            alpha = jnp.where(active, norm_next / curv, 0.0)
            scal[1, c] = alpha
            scal[2, c] = scal[2, c] + alpha * norm_next
        return carry

    lax.fori_loop(1, MICRO_MAX, iterate, 0)

    scale = 1.0 / (VOX * YZ)
    face_totals = [total_of(part.get()) for part in face_sums]
    fields = [(face_totals[d] - scal[2, d]) * scale for d in range(3)] + coarse
    slot = ((lane >> 3) - col) & 15
    packed = fields[4]
    for f in range(4):
        packed = jnp.where(slot == f, fields[f], packed)
    mine[...] = packed[0:1]

    me = col * nrow + row
    pl.semaphore_wait(barrier, n - 1)
    got[pl.ds(me, 1)] = packed[0:1]
    for offset in offsets:
        pltpu.make_async_remote_copy(
            src_ref=mine,
            dst_ref=got.at[pl.ds(me, 1)],
            send_sem=send_sem,
            recv_sem=recv_sem,
            device_id=peer_of(row, col, offset, nrow, ncol),
            device_id_type=pl.DeviceIdType.MESH,
        ).start()

    entries = {}
    for c in range(3):
        alpha = scal[1, c]
        sums = [Sum(2), Sum(2), Sum(2)]
        for xc in range(XC):
            for yc in range(YC):
                for zc in range(ZC):
                    at = (c, xc, yc, zc)
                    value = fluct[at] + alpha * direction[at]
                    turned[pl.ds(xc * HALF + yc * VOX + zc, 8, stride=3), :] = value
                    for d in range(3):
                        sums[d].add(value * rhs[d, xc, yc, zc])
        for d in range(3):
            entry = total_of(sums[d].get())
            entries[d, c] = ((face_totals[d] - entry) if d == c else -entry) * scale
        for xc in range(XC):
            for t, (start, size) in enumerate(SPANS):
                block = turned[xc * HALF + start : xc * HALF + start + size, :].T
                for xs in range(8):
                    for yh in range(2):
                        row = (xs * 2 + yh) * 8
                        piece = block[row : row + 8]
                        if size < 128:
                            piece = jnp.concatenate([piece, jnp.zeros((8, 128 - size), jnp.float32)], axis=1)
                        rows.at[t][pl.ds(yh * ELEMENTS * VOX + 3 * xs + xc, 8, stride=VOX), :] = piece
        for e in range(ELEMENTS):
            for yh in range(2):
                base = (yh * ELEMENTS + e) * VOX
                for t, (start, size) in enumerate(SPANS):
                    placed[e, c, :, yh * HALF + start : yh * HALF + start + size] = rows[
                        t, base : base + VOX, 0:size
                    ]


    for d in range(3):
        for c in range(3):
            tangent_ref[0, d, c] = entries[d, c][0:1, 0:ELEMENTS]

    stores = [pltpu.make_async_copy(placed.at[e], states_ref.at[0, 0, e], out_sems.at[e]) for e in range(ELEMENTS)]
    for copy in stores:
        copy.start()

    whole = pltpu.make_async_remote_copy(
        src_ref=got.at[pl.ds(0, n - 1)],
        dst_ref=got.at[pl.ds(0, n - 1)],
        send_sem=send_sem,
        recv_sem=recv_sem,
        device_id=peer_of(row, col, offsets[0], nrow, ncol),
        device_id_type=pl.DeviceIdType.MESH,
    )
    whole.wait_recv()
    group = lane >> 3
    for half in range(2):
        found = [jnp.zeros((8, 128), jnp.float32)] * 5
        for c in range(ncol // 2):
            block = got[8 * (half * (ncol // 2) + c) : 8 * (half * (ncol // 2) + c) + 8]
            for f in range(5):
                found[f] = jnp.where(group == (c + f) % 16, block, found[f])
        for f in range(5):
            table_ref[f, half] = found[f]
    whole.wait_send()
    for copy in stores:
        copy.wait()


def fused(phases, grain, phase_cond, counts, current, load, nrow, ncol):
    field = pltpu.VMEM((3, XC, YC, ZC, 8, 128), jnp.float32)
    vmem = pl.BlockSpec(memory_space=pltpu.VMEM)
    return pl.pallas_call(
        functools.partial(fused_kernel, nrow, ncol),
        out_shape=(
            jax.ShapeDtypeStruct((1, 1, ELEMENTS, 3, VOX, YZ), jnp.float32),
            jax.ShapeDtypeStruct((1, 3, 3, 1, ELEMENTS), jnp.float32),
            jax.ShapeDtypeStruct((5, 2, 8, 128), jnp.float32),
        ),
        in_specs=[pl.BlockSpec(memory_space=pltpu.HBM)] * 6,
        out_specs=(pl.BlockSpec(memory_space=pltpu.HBM), vmem, vmem),
        scratch_shapes=[
            pltpu.VMEM(phases.shape, jnp.int32),
            pltpu.VMEM(grain.shape, jnp.float32),
            pltpu.SMEM(phase_cond.shape, jnp.float32),
            pltpu.SMEM(counts.shape, jnp.int32),
            pltpu.SMEM(current.shape, jnp.float32),
            pltpu.SMEM(load.shape, jnp.float32),
            pltpu.SemaphoreType.DMA((ELEMENTS + 4,)),
            pltpu.VMEM((YC, ZC, 8, 128), jnp.float32),
            pltpu.VMEM((ELEMENTS, 3, VOX, YZ), jnp.float32),
            pltpu.SemaphoreType.DMA((ELEMENTS,)),
            pltpu.VMEM((3, 2 * ELEMENTS * VOX, 128), jnp.float32),
            pltpu.VMEM((XC * HALF, 128), jnp.float32),
            pltpu.VMEM((XC, YC, ZC, 8, 128), jnp.float32),
            field, field, field, field, field, field,
            pltpu.VMEM((3, 3, 8, 128), jnp.float32),
            pltpu.VMEM((1, 128), jnp.float32),
            pltpu.VMEM((nrow * ncol, 128), jnp.float32),
            pltpu.SemaphoreType.DMA,
            pltpu.SemaphoreType.DMA,
        ],
        compiler_params=pltpu.CompilerParams(collective_id=0, has_side_effects=True),
        name="fused",
    )(phases, grain, phase_cond, counts, current, load)


def coarse_kernel(ncol, table_ref, tangent_in, states_in, inc_ref, res_ref, tangent_ref, states_ref, held, in_sems, out_sems):
    loads = [pltpu.make_async_copy(states_in.at[0, 0, e], held.at[e], in_sems.at[e]) for e in range(ELEMENTS)]
    stores = [pltpu.make_async_copy(held.at[e], states_ref.at[0, 0, e], out_sems.at[e]) for e in range(ELEMENTS)]
    for copy in loads:
        copy.start()
    tangent_ref[...] = tangent_in[...]

    lane = lax.broadcasted_iota(jnp.int32, (8, 128), 1)
    ex = lax.broadcasted_iota(jnp.int32, (8, 128), 0)
    group, ez = lane >> 3, lane & 7

    def field(f):
        return [pltpu.roll(table_ref[f, h], (128 - 8 * f) % 128, 1) for h in range(2)]

    def x_up(v):
        return [pltpu.roll(part, 7, 0) for part in v]

    def x_down(v):
        return [pltpu.roll(part, 1, 0) for part in v]

    def y_up(v):
        first, second = (pltpu.roll(part, 120, 1) for part in v)
        return [jnp.where(group < 15, first, second), second]

    def y_down(v):
        first, second = (pltpu.roll(part, 8, 1) for part in v)
        return [first, jnp.where(group > 0, second, first)]

    def z_up(v):
        return [pltpu.roll(part, 127, 1) for part in v]

    def z_down(v):
        return [pltpu.roll(part, 1, 1) for part in v]

    yes = ex >= 0
    moves = (
        (0, x_up, [ex < 7] * 2), (0, x_down, [ex > 0] * 2),
        (1, y_up, [yes, group < 15]), (1, y_down, [group > 0, yes]),
        (2, z_up, [ez < 7] * 2), (2, z_down, [ez > 0] * 2),
    )
    centre = [jnp.zeros((8, 128), jnp.float32)] * 2
    weights = []
    kd = [field(d) for d in range(3)]
    for d, move, has in moves:
        other = move(kd[d])
        pair = [0.5 * (own + jnp.where(ok, far, 0.0)) for own, far, ok in zip(kd[d], other, has)]
        centre = [c + p for c, p in zip(centre, pair)]
        weights.append([jnp.where(ok, p, 0.0) for p, ok in zip(pair, has)])

    def apply(v):
        moved = [move(v) for _, move, _ in moves]
        out = []
        for h in range(2):
            parts = [weights[i][h] * moved[i][h] for i in range(6)]
            out.append(centre[h] * v[h] - ((parts[0] + parts[1]) + (parts[2] + parts[3]) + (parts[4] + parts[5])))
        return out

    def total(u, v):
        value = u[0] * v[0] + u[1] * v[1]
        for shift in (1, 2, 4):
            value = value + pltpu.roll(value, shift, 0)
        return jnp.sum(value, axis=1, keepdims=True)

    def axpy(a, u, v):
        return [a * p + q for p, q in zip(u, v)]

    image = apply(field(3))
    residual = [p - q for p, q in zip(field(4), image)]
    image = apply(residual)
    increment = older = alpha = None
    for i in range(MACRO_ITERS):
        gamma, delta = total(residual, residual), total(image, residual)
        deep = apply(image) if i < MACRO_ITERS - 1 else None
        if i == 0:
            alpha = gamma / delta
            p, s, z = residual, image, deep
            increment = [alpha * v for v in p]
        else:
            beta = gamma / older
            alpha = gamma / (delta - beta * gamma / alpha)
            p, s = axpy(beta, p, residual), axpy(beta, s, image)
            z = axpy(beta, z, deep) if deep is not None else None
            increment = axpy(alpha, p, increment)
        older = gamma
        residual = axpy(-alpha, s, residual)
        if deep is not None:
            image = axpy(-alpha, z, image)
        if i == 1:
            for incoming, outgoing in zip(loads, stores):
                incoming.wait()
                outgoing.start()

    row, col = lax.axis_index("row"), lax.axis_index("col")
    for value, ref in ((increment, inc_ref), (residual, res_ref)):
        own = jnp.where(ex == row, jnp.where(col < 16, value[0], value[1]), 0.0)
        own = jnp.where(group == (col & 15), own, 0.0)
        for shift in (1, 2, 4):
            own = own + pltpu.roll(own, shift, 0)
        own = pltpu.roll(own, (128 - 8 * (col & 15)) & 127, 1)
        ref[0] = own[0:1, 0:ELEMENTS]
    for outgoing in stores:
        outgoing.wait()


def coarse(table, tangent, states, ncol):
    vmem = pl.BlockSpec(memory_space=pltpu.VMEM)
    anywhere = pl.BlockSpec(memory_space=pl.ANY)
    small = jax.ShapeDtypeStruct((1, 1, ELEMENTS), jnp.float32)
    return pl.pallas_call(
        functools.partial(coarse_kernel, ncol),
        out_shape=(
            small, small,
            jax.ShapeDtypeStruct(tangent.shape, jnp.float32),
            jax.ShapeDtypeStruct(states.shape, jnp.float32),
        ),
        in_specs=[vmem, vmem, anywhere],
        out_specs=(vmem, vmem, vmem, anywhere),
        scratch_shapes=[
            pltpu.VMEM((ELEMENTS, 3, VOX, YZ), jnp.float32),
            pltpu.SemaphoreType.DMA((ELEMENTS,)),
            pltpu.SemaphoreType.DMA((ELEMENTS,)),
        ],
        name="coarse",
    )(table, tangent, states)


def shards(nrow, ncol, phases, grain, phase_cond, micro_counts, current, load):
    states, tangent, table = fused(phases, grain, phase_cond, micro_counts, current, load, nrow, ncol)
    increment, residual, tangent, states = coarse(table, tangent, states, ncol)
    return (states, tangent.transpose(0, 3, 4, 1, 2), increment, residual)


def solution(mesh):
    placed = (
        P("row", "col", None, None, None),
        P("row", "col", None, None, None),
        P(),
        P("row", "col", None),
        P("row", "col", None),
        P("row", "col", None),
    )
    return jax.shard_map(
        functools.partial(shards, mesh.shape["row"], mesh.shape["col"]),
        mesh=mesh,
        in_specs=placed,
        out_specs=(
            P("row", "col", None, None, None, None),
            P("row", "col", None, None, None),
            P("row", "col", None),
            P("row", "col", None),
        ),
        check_vma=False,
    )
```
